32 devices in a mesh: leaf: 8 (over z, core), grp: 4 (over y, x).
Axes of the slice: x: 2, y: 2, z: 4, core: 2. Of those that a mesh axis runs over, the one named last changes fastest.
Arguments:
- front_rows: bfloat16 [8192, 6144], P('leaf', 'grp'), may hold values from -0.078125 to 0.078125
- sample_matrix: bfloat16 [6144, 1024], P('grp'), may hold values from -6 to 6
- pivots: int32 [15, 512], replicated, may hold values from 0 to 1023, as said below
Outputs:
- bases: float32 [4, 8, 1024, 512], P(None, 'leaf', 'grp')
- top_sample: float32 [1024, 512], P('grp')
The draws below stay inside these ranges and needn't reach their ends.
Inputs may be any that keep to these rules, and one draw needn't show every extreme that they name: `pivots`: row o_l + j (o_l = 2 * 8 - 2 * 8 / 2^l) holds node j of level l: 512 distinct column numbers of its 1024 columns; entries k * 128 to (k + 1) * 128 - 1 lie in k * 256 to (k + 1) * 256 - 1.
All inputs are finite; a program needn't handle non-finite values.
Results may differ from the reference program's by a relative error of at most 0.0003.
Values sent between devices are 32-bit elements; how exact they have to be, the bound alone decides.
A program may use at most 128 MiB of HBM per device.

```python
import jax
import jax.numpy as jnp
from jax import lax

R = 512
K = 1024
LEAVES = 8
MERGES = 3
NODES = 15
COLS = 6144
ROWS_DEV = 256
PIV_DEV = 128


def draw_pivots(key, part):
    blocks = 2 * R // ROWS_DEV
    keys = jax.random.split(jax.random.fold_in(key, 17), NODES * blocks)
    orders = jax.vmap(lambda single: jax.random.permutation(single, ROWS_DEV))(keys)
    picked = orders[:, :PIV_DEV].astype(jnp.int32).reshape(NODES, blocks, PIV_DEV)
    starts = (jnp.arange(blocks, dtype=jnp.int32) * ROWS_DEV)[None, :, None]
    return (picked + starts).reshape(NODES, R).astype(jnp.int32)


def shard_levels(key, shape, cuts, least, high):
    gain = 1.0
    for dim, parts in cuts:
        draws = jax.random.uniform(jax.random.fold_in(jax.random.fold_in(key, 6), dim), (parts,), jnp.float32, least / len(cuts), high / len(cuts))
        gain = gain * jnp.repeat(jnp.exp(draws), shape[dim] // parts).reshape((-1,) + (1,) * (len(shape) - 1 - dim))
    return gain


def noise(own_key, shape, scale, reach, cuts=(), kind=jnp.bfloat16):
    result = scale * jax.random.normal(own_key, shape, jnp.float32)
    if cuts:
        result = result * shard_levels(own_key, shape, cuts, -0.22, 0.18)
    return jnp.clip(result, -reach, reach).astype(kind)


def setup_inputs(seed: int = 0) -> dict:
    splits = jax.random.split(jax.random.key(seed), 4)
    front_rows = noise(splits[0], (LEAVES * 2 * R, COLS), COLS ** -0.5, 0.078125, ((0, 8), (1, 4)))
    sample_matrix = noise(splits[1], (COLS, K), 1.0, 6.0, ((0, 4),))
    pivots = draw_pivots(jax.random.fold_in(splits[3], 71), 0)
    return {"front_rows": front_rows, "sample_matrix": sample_matrix, "pivots": pivots}


def solve_basis(gram, cross):
    factor = jnp.linalg.cholesky(gram)
    identity = jnp.eye(gram.shape[0], dtype=gram.dtype)
    inverse_factor = jax.scipy.linalg.solve_triangular(factor, identity, lower=True)
    gram_inverse = jnp.dot(inverse_factor.T.astype(jnp.float32), inverse_factor.astype(jnp.float32), precision=lax.Precision.HIGHEST, preferred_element_type=jnp.float32)
    return jnp.dot(cross.astype(jnp.float32), gram_inverse.astype(jnp.float32), precision=lax.Precision.HIGHEST, preferred_element_type=jnp.float32)

def reference(front_rows, sample_matrix, pivots):

    def first_sample(block):
        return lax.dot_general(sample_matrix.astype(jnp.float32), block.astype(jnp.float32), (((0,), (1,)), ((), ())), preferred_element_type=jnp.float32)
    samples = lax.map(first_sample, front_rows.reshape(LEAVES, 2 * R, COLS))

    def one_node(packed):
        sample, chosen = packed
        skeleton = jnp.take(sample, chosen, axis=1)
        gram = lax.dot_general(skeleton.astype(jnp.float32), skeleton.astype(jnp.float32), (((0,), (0,)), ((), ())), precision=lax.Precision.HIGHEST, preferred_element_type=jnp.float32)
        cross = lax.dot_general(sample.astype(jnp.float32), skeleton.astype(jnp.float32), (((0,), (0,)), ((), ())), precision=lax.Precision.HIGHEST, preferred_element_type=jnp.float32)
        return (solve_basis(gram, cross), skeleton)
    collected = []
    offset = 0
    skeletons = samples
    for depth_level in range(MERGES + 1):
        nodes_now = LEAVES >> depth_level
        chosen = pivots[offset:offset + nodes_now]
        node_bases, skeletons = lax.map(one_node, (samples, chosen))
        collected.append(jnp.repeat(node_bases, 2 ** depth_level, axis=0))
        offset = offset + nodes_now
        if depth_level < MERGES:
            paired = skeletons.reshape(nodes_now // 2, 2, K, R)
            samples = jnp.concatenate([paired[:, 0], paired[:, 1]], axis=2)
    return (jnp.stack(collected), skeletons[0])
```

```python
import functools

import jax
import jax.numpy as jnp
from jax import lax
from jax.experimental import pallas as pl
from jax.experimental.pallas import tpu as pltpu
from jax.sharding import PartitionSpec as P

COARSE_CAP = 24
FINE_CAP = 6
COARSE_GOAL = 1e-2
FINE_GOAL = 1e-6


def from_partner(x, axis, mask):
    return lax.ppermute(x, axis, [(i, i ^ mask) for i in range(lax.axis_size(axis))])


def halves(x):
    high = x.astype(jnp.bfloat16)
    return high, (x - high.astype(jnp.float32)).astype(jnp.bfloat16)


def mul(a, b):
    return jnp.dot(a, b, preferred_element_type=jnp.float32)


def mul_t(a, b):
    return lax.dot_general(
        a, b, (((1,), (1,)), ((), ())), preferred_element_type=jnp.float32
    )


def inverse_kernel(skeleton_ref, out_ref, scaled, high, low, inv, swept):
    size = out_ref.shape[0]
    rows = lax.broadcasted_iota(jnp.int32, (size, size), 0)
    lanes = lax.broadcasted_iota(jnp.int32, (size, size), 1)
    diagonal = rows == lanes
    q_high, q_low = halves(skeleton_ref[...])
    gram = mul_t(q_high, q_high) + (mul_t(q_high, q_low) + mul_t(q_low, q_high))
    only = jnp.where(diagonal, gram, 0.0)
    by_lane = lax.rsqrt(jnp.sum(only, axis=0, keepdims=True))
    by_row = lax.rsqrt(jnp.sum(only, axis=1, keepdims=True))
    matrix = gram * by_lane * by_row
    scaled[...] = matrix
    m_high, m_low = halves(matrix)
    high[...] = m_high
    low[...] = m_low
    start = 1.0 / jnp.max(jnp.sum(jnp.abs(matrix), axis=0, keepdims=True))
    inv[...] = jnp.where(diagonal, 2.0 * start, 0.0) - (start * start) * matrix

    def coarse(carry):
        step, _ = carry
        now = inv[...]
        now_high = now.astype(jnp.bfloat16)
        gap = jnp.where(diagonal, 1.0, 0.0) - mul(high[...], now_high)
        inv[...] = now + mul(now_high, gap.astype(jnp.bfloat16))
        return step + 1, jnp.sum(gap * gap)

    def coarse_more(carry):
        step, error = carry
        return (step < COARSE_CAP) & (error > COARSE_GOAL)

    lax.while_loop(coarse_more, coarse, (jnp.int32(0), jnp.float32(1e9)))

    def fine(carry):
        step, _ = carry
        now = inv[...]
        now_high, now_low = halves(now)
        product = mul(high[...], now_high) + (
            mul(low[...], now_high) + mul(high[...], now_low)
        )
        gap = jnp.where(diagonal, 1.0, 0.0) - product
        inv[...] = now + mul(now_high, gap.astype(jnp.bfloat16))
        return step + 1, jnp.sum(gap * gap)

    def fine_more(carry):
        step, error = carry
        return (step < FINE_CAP) & (error > FINE_GOAL)

    _, last = lax.while_loop(fine_more, fine, (jnp.int32(0), jnp.float32(1e9)))
    good = last <= FINE_GOAL

    @pl.when(good)
    def _():
        out_ref[...] = inv[...] * by_lane * by_row

    @pl.when(jnp.logical_not(good))
    def _():
        swept[...] = scaled[...]

        def sweep(k, carry):
            now = swept[...]
            row = jnp.sum(jnp.where(rows == k, now, 0.0), axis=0, keepdims=True)
            col = jnp.sum(jnp.where(lanes == k, now, 0.0), axis=1, keepdims=True)
            pivot = jnp.sum(
                jnp.where(lanes[:1] == k, row, 0.0), axis=1, keepdims=True
            )
            over = 1.0 / pivot
            updated = now - (col * over) * row
            updated = jnp.where(rows == k, row * over, updated)
            updated = jnp.where(lanes == k, col * over, updated)
            swept[...] = jnp.where((rows == k) & (lanes == k), -over, updated)
            return carry

        lax.fori_loop(0, size, sweep, 0)
        out_ref[...] = -swept[...] * by_lane * by_row


def gram_inverse(skeleton_t):
    size, depth = skeleton_t.shape
    return pl.pallas_call(
        inverse_kernel,
        out_shape=jax.ShapeDtypeStruct((size, size), jnp.float32),
        in_specs=[pl.BlockSpec(memory_space=pltpu.VMEM)],
        out_specs=pl.BlockSpec(memory_space=pltpu.VMEM),
        scratch_shapes=[
            pltpu.VMEM((size, size), jnp.float32),
            pltpu.VMEM((size, size), jnp.bfloat16),
            pltpu.VMEM((size, size), jnp.bfloat16),
            pltpu.VMEM((size, size), jnp.float32),
            pltpu.VMEM((size, size), jnp.float32),
        ],
        compiler_params=pltpu.CompilerParams(vmem_limit_bytes=40 * 1024 * 1024),
        cost_estimate=pl.CostEstimate(
            flops=2 * size * size * (3 * depth + 36 * size),
            bytes_accessed=4 * size * (size + depth),
            transcendentals=0,
        ),
        name="gram_inverse",
    )(skeleton_t)


def apply_basis(row_block, skeleton_t, inverse):
    cross = lax.dot_general(
        row_block,
        skeleton_t,
        (((1,), (1,)), ((), ())),
        precision=lax.Precision.HIGH,
        preferred_element_type=jnp.float32,
    )
    return jnp.dot(
        cross,
        inverse,
        precision=lax.Precision.HIGH,
        preferred_element_type=jnp.float32,
    )


def take_rows(x, index):
    return x.at[index].get(mode="promise_in_bounds")


def on_device(front_rows, sample_matrix, pivots):
    leaf_count = lax.axis_size("leaf")
    grp_count = lax.axis_size("grp")
    merges = leaf_count.bit_length() - 1
    leaf_index = lax.axis_index("leaf")
    grp_index = lax.axis_index("grp")
    node_rows = front_rows.shape[0]
    rank_size = pivots.shape[1]
    cols_dev = sample_matrix.shape[1] // grp_count
    rows_dev = node_rows // grp_count
    piv_dev = rank_size // grp_count
    half = rank_size // 2
    row_block = lax.psum_scatter(
        jnp.dot(front_rows, sample_matrix, preferred_element_type=jnp.float32),
        "grp",
        scatter_dimension=0,
        tiled=True,
    )

    def node_pivots(level):
        offset = 2 * leaf_count - (2 * leaf_count >> level)
        return lax.dynamic_index_in_dim(
            pivots, offset + (leaf_index >> level), 0, keepdims=False
        )

    local = lax.dynamic_slice_in_dim(node_pivots(0), grp_index * piv_dev, piv_dev)
    picked = take_rows(row_block, local - grp_index * rows_dev)
    skeletons = [lax.all_gather(picked, "grp", axis=0, tiled=True)]
    blocks = [row_block]
    wanted_side = grp_index // (grp_count // 2)
    for level in range(1, merges + 1):
        below = skeletons[-1]
        bit = level - 1
        side = (leaf_index >> bit) % 2
        mine = lax.dynamic_slice_in_dim(node_pivots(level), side * half, half)
        mine = take_rows(below, mine - side * rank_size)
        other = from_partner(mine, "leaf", 1 << bit)
        upper = jnp.where(side == 0, mine, other)
        lower = jnp.where(side == 0, other, mine)
        skeletons.append(jnp.concatenate([upper, lower], axis=0))
        piece = lax.dynamic_slice_in_dim(
            below, grp_index % (grp_count // 2) * rows_dev, rows_dev, 0
        )
        partner = from_partner(piece, "leaf", 1 << bit)
        blocks.append(jnp.where(side == wanted_side, piece, partner))
    collected = [
        apply_basis(block, skeleton, gram_inverse(skeleton))
        for block, skeleton in zip(blocks, skeletons)
    ]
    top = lax.dynamic_slice_in_dim(skeletons[-1], grp_index * cols_dev, cols_dev, 1).T
    return (jnp.stack(collected)[:, None], top)


def solution(mesh):
    placed = (P("leaf", "grp"), P("grp", None), P())
    return jax.shard_map(
        on_device,
        mesh=mesh,
        in_specs=placed,
        out_specs=(P(None, "leaf", "grp", None), P("grp", None)),
        check_vma=False,
    )
```

```python
import functools

import jax
import jax.numpy as jnp
from jax import lax
from jax.experimental import pallas as pl
from jax.experimental.pallas import tpu as pltpu
from jax.sharding import PartitionSpec as P

COARSE_CAP = 24
FINE_CAP = 6
COARSE_GOAL = 1e-2
FINE_GOAL = 1e-6


def from_partner(x, axis, mask):
    return lax.ppermute(x, axis, [(i, i ^ mask) for i in range(lax.axis_size(axis))])


def halves(x):
    high = x.astype(jnp.bfloat16)
    return high, (x - high.astype(jnp.float32)).astype(jnp.bfloat16)


def mul(a, b):
    return jnp.dot(a, b, preferred_element_type=jnp.float32)


def mul_t(a, b):
    return lax.dot_general(
        a, b, (((1,), (1,)), ((), ())), preferred_element_type=jnp.float32
    )


def inverse_kernel(skeleton_ref, out_ref, scaled, high, low, inv, swept):
    size = out_ref.shape[0]
    rows = lax.broadcasted_iota(jnp.int32, (size, size), 0)
    lanes = lax.broadcasted_iota(jnp.int32, (size, size), 1)
    diagonal = rows == lanes
    q_high, q_low = halves(skeleton_ref[...])
    gram = mul_t(q_high, q_high) + (mul_t(q_high, q_low) + mul_t(q_low, q_high))
    only = jnp.where(diagonal, gram, 0.0)
    by_lane = lax.rsqrt(jnp.sum(only, axis=0, keepdims=True))
    by_row = lax.rsqrt(jnp.sum(only, axis=1, keepdims=True))
    matrix = gram * by_lane * by_row
    scaled[...] = matrix
    m_high, m_low = halves(matrix)
    high[...] = m_high
    low[...] = m_low
    square = mul(m_high, m_high)
    start = 1.8 * lax.rsqrt(jnp.max(jnp.sum(jnp.abs(square), axis=0, keepdims=True)))
    inv[...] = jnp.where(diagonal, 2.0 * start, 0.0) - (start * start) * matrix

    def coarse(carry):
        step, _ = carry
        now = inv[...]
        now_high = now.astype(jnp.bfloat16)
        gap = jnp.where(diagonal, 1.0, 0.0) - mul(high[...], now_high)
        inv[...] = now + mul(now_high, gap.astype(jnp.bfloat16))
        return step + 1, jnp.sum(gap * gap)

    def coarse_more(carry):
        step, error = carry
        return (step < COARSE_CAP) & (error > COARSE_GOAL)

    lax.while_loop(coarse_more, coarse, (jnp.int32(0), jnp.float32(1e9)))

    def fine(carry):
        step, _ = carry
        now = inv[...]
        now_high, now_low = halves(now)
        product = mul(high[...], now_high) + (
            mul(low[...], now_high) + mul(high[...], now_low)
        )
        gap = jnp.where(diagonal, 1.0, 0.0) - product
        inv[...] = now + mul(now_high, gap.astype(jnp.bfloat16))
        return step + 1, jnp.sum(gap * gap)

    def fine_more(carry):
        step, error = carry
        return (step < FINE_CAP) & (error > FINE_GOAL)

    _, last = lax.while_loop(fine_more, fine, (jnp.int32(0), jnp.float32(1e9)))
    good = last <= FINE_GOAL

    @pl.when(good)
    def _():
        out_ref[...] = inv[...] * by_lane * by_row

    @pl.when(jnp.logical_not(good))
    def _():
        swept[...] = scaled[...]

        def sweep(k, carry):
            now = swept[...]
            row = jnp.sum(jnp.where(rows == k, now, 0.0), axis=0, keepdims=True)
            col = jnp.sum(jnp.where(lanes == k, now, 0.0), axis=1, keepdims=True)
            pivot = jnp.sum(
                jnp.where(lanes[:1] == k, row, 0.0), axis=1, keepdims=True
            )
            over = 1.0 / pivot
            updated = now - (col * over) * row
            updated = jnp.where(rows == k, row * over, updated)
            updated = jnp.where(lanes == k, col * over, updated)
            swept[...] = jnp.where((rows == k) & (lanes == k), -over, updated)
            return carry

        lax.fori_loop(0, size, sweep, 0)
        out_ref[...] = -swept[...] * by_lane * by_row


def gram_inverse(skeleton_t):
    size, depth = skeleton_t.shape
    return pl.pallas_call(
        inverse_kernel,
        out_shape=jax.ShapeDtypeStruct((size, size), jnp.float32),
        in_specs=[pl.BlockSpec(memory_space=pltpu.VMEM)],
        out_specs=pl.BlockSpec(memory_space=pltpu.VMEM),
        scratch_shapes=[
            pltpu.VMEM((size, size), jnp.float32),
            pltpu.VMEM((size, size), jnp.bfloat16),
            pltpu.VMEM((size, size), jnp.bfloat16),
            pltpu.VMEM((size, size), jnp.float32),
            pltpu.VMEM((size, size), jnp.float32),
        ],
        compiler_params=pltpu.CompilerParams(vmem_limit_bytes=40 * 1024 * 1024),
        cost_estimate=pl.CostEstimate(
            flops=2 * size * size * (3 * depth + 36 * size),
            bytes_accessed=4 * size * (size + depth),
            transcendentals=0,
        ),
        name="gram_inverse",
    )(skeleton_t)


def cross_of(row_block, skeleton_t):
    return lax.dot_general(
        row_block,
        skeleton_t,
        (((1,), (1,)), ((), ())),
        precision=lax.Precision.HIGH,
        preferred_element_type=jnp.float32,
    )


def apply_inverse(cross, inverse):
    return jnp.dot(
        cross,
        inverse,
        precision=lax.Precision.HIGH,
        preferred_element_type=jnp.float32,
    )


def take_rows(x, index):
    return x.at[index].get(mode="promise_in_bounds")


def bit_of(index, bit):
    return (index >> bit) % 2


def in_order(mine, other, second, axis):
    first = jnp.where(second == 0, mine, other)
    last = jnp.where(second == 0, other, mine)
    return jnp.concatenate([first, last], axis=axis)


def scatter_sum(parts, index, axis, bits, order):
    rows = parts.shape[0] >> bits
    width = parts.shape[1]
    parts = parts.reshape((2,) * bits + (rows, width))
    for bit in order:
        dim = bits - 1 - bit
        own = bit_of(index, bit)
        kept = lax.dynamic_slice_in_dim(parts, own, 1, dim)
        sent = lax.dynamic_slice_in_dim(parts, 1 - own, 1, dim)
        parts = kept + from_partner(sent, axis, 1 << bit)
    return parts.reshape(rows, width)


def gather_rows(block, index, axis, bits, order):
    rows, width = block.shape
    whole = block.reshape((1,) * bits + (rows, width))
    for bit in order:
        other = from_partner(whole, axis, 1 << bit)
        whole = in_order(whole, other, bit_of(index, bit), bits - 1 - bit)
    return whole.reshape(rows << bits, width)


def fetch(x, leaf_index, bit):
    if bit < 2:
        return from_partner(x, "leaf", 1 << bit)
    core = leaf_index % 2
    rows = x.shape[0] // 2
    part = lax.dynamic_slice_in_dim(x, core * rows, rows, 0)
    part = from_partner(part, "leaf", 1 << bit)
    return in_order(part, from_partner(part, "leaf", 1), core, 0)


def on_device(front_rows, sample_matrix, pivots):
    leaf_count = lax.axis_size("leaf")
    grp_count = lax.axis_size("grp")
    merges = leaf_count.bit_length() - 1
    grp_bits = grp_count.bit_length() - 1
    leaf_index = lax.axis_index("leaf")
    grp_index = lax.axis_index("grp")
    node_rows = front_rows.shape[0]
    rank_size = pivots.shape[1]
    depth = sample_matrix.shape[1]
    cols_dev = depth // grp_count
    rows_dev = node_rows // grp_count
    piv_dev = rank_size // grp_count
    half = rank_size // 2

    def node_pivots(level):
        offset = 2 * leaf_count - (2 * leaf_count >> level)
        return lax.dynamic_index_in_dim(
            pivots, offset + (leaf_index >> level), 0, keepdims=False
        )

    local = lax.dynamic_slice_in_dim(node_pivots(0), grp_index * piv_dev, piv_dev)
    local = local - grp_index * rows_dev
    orders = (tuple(range(grp_bits)), tuple(range(grp_bits))[::-1])
    width = depth // len(orders)
    sums, gathered = [], []
    for number, order in enumerate(orders):
        columns = sample_matrix[:, number * width : (number + 1) * width]
        part = jnp.dot(front_rows, columns, preferred_element_type=jnp.float32)
        part = scatter_sum(part, grp_index, "grp", grp_bits, order)
        sums.append(part)
        picked = take_rows(part, local)
        gathered.append(gather_rows(picked, grp_index, "grp", grp_bits, order))
    row_block = jnp.concatenate(sums, axis=1)
    skeletons = [jnp.concatenate(gathered, axis=1)]
    wanted_side = grp_index // (grp_count // 2)
    for level in range(1, merges + 1):
        below = skeletons[-1]
        side = bit_of(leaf_index, level - 1)
        mine = lax.dynamic_slice_in_dim(node_pivots(level), side * half, half)
        mine = take_rows(below, mine - side * rank_size)
        other = fetch(mine, leaf_index, level - 1)
        skeletons.append(in_order(mine, other, side, 0))
    crosses = [cross_of(row_block, skeletons[0])]
    for level in range(1, merges + 1):
        side = bit_of(leaf_index, level - 1)
        piece = lax.dynamic_slice_in_dim(
            skeletons[level - 1], grp_index % (grp_count // 2) * rows_dev, rows_dev, 0
        )
        cross = cross_of(piece, skeletons[level])
        other = from_partner(cross, "leaf", 1 << (level - 1))
        crosses.append(jnp.where(side == wanted_side, cross, other))
    collected = [
        apply_inverse(cross, gram_inverse(skeleton))
        for cross, skeleton in zip(crosses, skeletons)
    ]
    top = lax.dynamic_slice_in_dim(skeletons[-1], grp_index * cols_dev, cols_dev, 1).T
    return (jnp.stack(collected)[:, None], top)


def solution(mesh):
    placed = (P("leaf", "grp"), P("grp", None), P())
    return jax.shard_map(
        on_device,
        mesh=mesh,
        in_specs=placed,
        out_specs=(P(None, "leaf", "grp", None), P("grp", None)),
        check_vma=False,
    )
```
